32 devices in a mesh: hid: 8 (over z, y), col: 4 (over x, core).
Axes of the slice: x: 2, y: 2, z: 4, core: 2. Of those that a mesh axis runs over, the one named last changes fastest.
Arguments:
- inputs: bfloat16 [3840, 28672], P('col', 'hid'), may hold values from -6 to 6
- out_grads: bfloat16 [3840, 8192], P('col', 'hid'), may hold values from -6 to 6
- proj_in: bfloat16 [96, 28672], P(None, 'hid'), may hold values from -0.03125 to 0.03125
- proj_out: bfloat16 [192, 8192], P(None, 'hid'), may hold values from -0.0625 to 0.0625
- curvature: bfloat16 [18432, 18432], P('hid', 'col'), may hold values from -0.119628906 to 0.119628906
Outputs:
- applied: float32 [120, 18432], P('hid', 'col')
- curvature_new: bfloat16 [18432, 18432], P('hid', 'col')
The draws below stay inside these ranges and needn't reach their ends.
All inputs are finite; a program needn't handle non-finite values.
Results may differ from the reference program's by a relative error of at most 0.012.
Values may be sent and summed in bfloat16 or wider, within the bound.
No kernel may reach another device: no remote copies, remote signals or barrier semaphores. Data moves between devices by JAX's collectives and lax.ppermute only.
A program may use at most 128 MiB of HBM per device.

```python
import jax
import jax.numpy as jnp
from jax import lax

HIDDEN_SIZE = 28672
DMODEL = 8192
PIN = 96
POUT = 192
SEQ = 32
RANK = 18432
TOKENS = 3840
N_HID = 8


def block_scale(own_key, shape, shards, least, high):
    factor_of = 1.0
    for position, shards_of in shards:
        draws = jax.random.uniform(jax.random.fold_in(jax.random.fold_in(own_key, 6), position), (shards_of,), jnp.float32, least / len(shards), high / len(shards))
        factor_of = factor_of * jnp.repeat(jnp.exp(draws), shape[position] // shards_of).reshape((-1,) + (1,) * (len(shape) - 1 - position))
    return factor_of


def noise(key, dims, spread, bound, cuts=(), kind=jnp.bfloat16):
    array = jax.random.normal(key, dims, jnp.float32) * spread
    if len(cuts) > 0:
        array = block_scale(key, dims, cuts, -0.22, 0.18) * array
    return jnp.clip(array, min=-bound, max=bound).astype(kind)


def setup_inputs(seed: int = 0) -> dict:
    streams_of = jax.random.split(jax.random.key(seed), 6)
    inputs = noise(streams_of[0], (TOKENS, HIDDEN_SIZE), 1.0, 6.0, ((0, 4), (1, 8)))
    out_grads = noise(streams_of[1], (TOKENS, DMODEL), 1.0, 6.0, ((0, 4), (1, 8)))
    proj_in = noise(streams_of[2], (PIN, HIDDEN_SIZE), HIDDEN_SIZE ** -0.5, 0.03125, ((1, 8),))
    proj_out = noise(streams_of[3], (POUT, DMODEL), DMODEL ** -0.5, 0.0625, ((1, 8),))
    curvature = noise(streams_of[4], (RANK, RANK), 0.02, 0.119628906, ((0, 8), (1, 4)))
    return dict(inputs=inputs, out_grads=out_grads, proj_in=proj_in, proj_out=proj_out, curvature=curvature)


gram_weight = 1.0 / 64.0
apply_weight = 1.0 / 16.0


def reference(inputs, out_grads, proj_in, proj_out, curvature):
    contract = (((1,), (1,)), ((), ()))
    feat = lax.dot_general(inputs, proj_in, contract, preferred_element_type=jnp.float32).astype(jnp.bfloat16)
    grad = lax.dot_general(out_grads, proj_out, contract, preferred_element_type=jnp.float32).astype(jnp.bfloat16)
    examples = feat.shape[0] // SEQ
    rows = jnp.einsum("eti,etj->eij", feat.reshape(examples, SEQ, PIN).astype(jnp.float32), grad.reshape(examples, SEQ, POUT).astype(jnp.float32))
    rows = rows.reshape(examples, RANK).astype(jnp.bfloat16)
    width = RANK // N_HID
    factor = gram_weight / examples

    def step(total, index):
        start = (index * width).astype(jnp.int32)
        left = lax.dynamic_slice_in_dim(rows, start, width, 1)
        stored = lax.dynamic_slice_in_dim(curvature, start, width, 0)
        gram = lax.dot_general(left, rows, (((0,), (0,)), ((), ())), preferred_element_type=jnp.float32)
        updated = (stored.astype(jnp.float32) + gram * factor).astype(jnp.bfloat16)
        total = total + jnp.dot(left, updated, preferred_element_type=jnp.float32)
        return total, updated

    total, blocks = lax.scan(step, jnp.zeros((examples, RANK), jnp.float32), jnp.arange(N_HID, dtype=jnp.int32))
    return total * apply_weight, blocks.reshape(RANK, RANK)
```

```python
import functools

import jax
import jax.numpy as jnp
from jax import lax
from jax.experimental import pallas as pl
from jax.experimental.pallas import tpu as pltpu
from jax.sharding import PartitionSpec as P

PIN = 96
POUT = 192
SEQ = 32
FEATURES = PIN + POUT
LANES = 128
PAIR = 2 * POUT
SUB = 16

gram_weight = 1.0 / 64.0
apply_weight = 1.0 / 16.0


f32 = jnp.float32
bf16 = jnp.bfloat16
CONTRACT_LAST = (((1,), (1,)), ((), ()))
VMEM = pltpu.VMEM


def chunk_of(width, parts):
    return width // parts if width % (parts * LANES) == 0 else width


def project_kernel(pieces, groups, split_first, x_ref, g_ref, pin_ref, pout_ref, *refs):
    outs, acc = refs[:-1], refs[-1]
    step = pl.program_id(0)
    tokens = x_ref.shape[0] // groups
    span = acc.shape[1] // groups

    @pl.when(step == 0)
    def _():
        acc[...] = jnp.zeros_like(acc)

    for q in range(groups):
        part = lax.dot_general(
            pin_ref[...], x_ref[q * tokens : (q + 1) * tokens], CONTRACT_LAST, preferred_element_type=f32
        )
        acc[POUT:, q * span : q * span + tokens] += part

    @pl.when(step < split_first)
    def _():
        for q in range(groups):
            part = lax.dot_general(
                pout_ref[...], g_ref[q * tokens : (q + 1) * tokens], CONTRACT_LAST, preferred_element_type=f32
            )
            acc[:POUT, q * span : q * span + tokens] += part

    @pl.when(step == pl.num_programs(0) - 1)
    def _():
        if pieces == 1:
            outs[0][...] = acc[...].astype(outs[0].dtype)
        else:
            me = lax.axis_index("hid")
            for d in range(pieces):
                at = pl.multiple_of((me ^ d) * LANES, LANES)
                outs[d][...] = acc[:, pl.ds(at, LANES)].astype(bf16)


def project(inputs, out_grads, proj_in, proj_out, lanes, groups, pieces):
    tokens, hidden = inputs.shape
    width = out_grads.shape[1]
    wide, narrow = chunk_of(hidden, 7), chunk_of(width, 4)
    steps, first = hidden // wide, width // narrow
    assert first <= steps
    out = (
        [jax.ShapeDtypeStruct((FEATURES, lanes), f32)]
        if pieces == 1
        else [jax.ShapeDtypeStruct((FEATURES, LANES), bf16)] * pieces
    )
    return pl.pallas_call(
        functools.partial(project_kernel, pieces, groups, first),
        grid=(steps,),
        in_specs=[
            pl.BlockSpec((tokens, wide), lambda k: (0, k)),
            pl.BlockSpec((tokens, narrow), lambda k: (0, jnp.minimum(k, first - 1))),
            pl.BlockSpec((PIN, wide), lambda k: (0, k)),
            pl.BlockSpec((POUT, narrow), lambda k: (0, jnp.minimum(k, first - 1))),
        ],
        out_specs=[pl.BlockSpec(o.shape, lambda k: (0, 0)) for o in out],
        out_shape=out,
        scratch_shapes=[VMEM((FEATURES, lanes), f32)],
        compiler_params=pltpu.CompilerParams(dimension_semantics=("arbitrary",)),
        name="project",
    )(inputs, out_grads, proj_in, proj_out)


def padded_pairs(count):
    return -(-count // 2)


def apply_kernel(parts, sizes, unit_row, own_half, refs_in, outs, scratch):
    k_count, n_count, factor, per_dest, absolute = sizes
    curv = refs_in[-1]
    rows_n_out, rows_kt_out, applied_outs = outs[0], outs[1], outs[2:]
    stage, weights, feats, rows, rk, rn, acc, sems = scratch
    chunks = stage.shape[0]
    chunk = stage.shape[2]

    def copy(j):
        return pltpu.make_async_copy(curv.at[:, pl.ds(j * chunk, chunk)], stage.at[j], sems.at[j])

    for j in range(chunks):
        copy(j).start()

    hid, col = lax.axis_index("hid"), lax.axis_index("col")
    half = own_half()
    lane = lax.broadcasted_iota(jnp.int32, (8, 2 * LANES), 1)
    sub = lax.broadcasted_iota(jnp.int32, (8, 2 * LANES), 0)
    side = (lane >= LANES).astype(jnp.int32)
    side = side + half - 2 * side * half
    belongs = sub == side * 4 + (lane % LANES) // SEQ
    mask = belongs.astype(f32)

    weights[...] = jnp.zeros_like(weights)
    k_pairs, n_pairs = padded_pairs(k_count), padded_pairs(n_count)

    def unit(a_ref, b_ref, j, row0):
        a, b = a_ref[j], b_ref[j]
        feats[:, :LANES] = a[POUT:].astype(f32)
        feats[:, LANES:] = b[POUT:].astype(f32)
        weights[64 : 64 + POUT, :LANES] = a[:POUT]
        weights[64 : 64 + POUT, LANES:] = b[:POUT]

        def tall(base, count, odd):
            got = []
            for p in range(padded_pairs(count)):
                i = 2 * p + odd
                if i < count:
                    got.append(jnp.broadcast_to(feats[pl.ds(base + i, 1), :], (8, 2 * LANES)) * mask)
                else:
                    got.append(jnp.zeros((8, 2 * LANES), f32))
            return got

        even = tall(hid * k_count, k_count, 0) + tall(col * n_count, n_count, 0)
        odd = tall(hid * k_count, k_count, 1) + tall(col * n_count, n_count, 1)
        even = jnp.concatenate(even, axis=0).astype(bf16)
        odd = jnp.concatenate(odd, axis=0).astype(bf16)
        left = lax.dot_general(even, weights[64:320], CONTRACT_LAST, preferred_element_type=f32)
        right = lax.dot_general(odd, weights[0:256], CONTRACT_LAST, preferred_element_type=f32)
        for p in range(k_pairs + n_pairs):
            le, ri = left[8 * p : 8 * p + 8], right[8 * p : 8 * p + 8]
            rows[pl.ds(row0, 8), PAIR * p : PAIR * p + LANES] = le[:, :LANES]
            rows[pl.ds(row0, 8), PAIR * p + LANES : PAIR * p + 2 * LANES] = le[:, LANES:] + ri[:, :LANES]
            rows[pl.ds(row0, 8), PAIR * p + 2 * LANES : PAIR * (p + 1)] = ri[:, LANES:]

    for at in range(parts):
        a_ref, b_ref = refs_in[2 * at], refs_in[2 * at + 1]

        @pl.loop(0, a_ref.shape[0])
        def _(j, at=at, a_ref=a_ref, b_ref=b_ref):
            unit(a_ref, b_ref, j, pl.multiple_of(8 * unit_row(at, j), 8))

    k_wide, n_wide = k_count * POUT, n_count * POUT
    rk[...] = rows[:, :k_wide].astype(bf16)
    rn[...] = rows[:, k_pairs * PAIR : k_pairs * PAIR + n_wide].astype(bf16)
    rows_n_out[...] = rn[...]
    rows_kt_out[...] = rk[...].T

    inner = lax.dot_general(rk[...], rk[...], CONTRACT_LAST, preferred_element_type=f32) * factor
    high = inner.astype(bf16)
    low = (inner - high.astype(f32)).astype(bf16)

    for j in range(chunks):
        at = slice(j * chunk, (j + 1) * chunk)
        near = rn[:, at]
        small = jnp.dot(high, near, preferred_element_type=f32) + jnp.dot(low, near, preferred_element_type=f32)
        copy(j).wait()
        big = jnp.dot(rk[...], stage[j], preferred_element_type=f32)
        acc[:, at] = (big + small) * apply_weight

    if absolute:
        applied_outs[0][...] = acc[...].astype(bf16).reshape(applied_outs[0].shape)
    else:
        for d in range(len(applied_outs)):
            start = pl.multiple_of((hid ^ d) * per_dest, 8)
            applied_outs[d][...] = acc[pl.ds(start, per_dest), :].astype(bf16)


def apply_rows(pairs, curvature, hid_count, slots, per_dest, factor, unit_row, own_half, absolute):
    k_wide, n_wide = curvature.shape
    k_count, n_count = k_wide // POUT, n_wide // POUT
    chunk = chunk_of(n_wide, 9)
    chunks = n_wide // chunk
    operands = [x for pair in pairs for x in pair]
    sizes = (k_count, n_count, factor, per_dest, absolute)
    outs = [jax.ShapeDtypeStruct((slots, n_wide), bf16), jax.ShapeDtypeStruct((k_wide, slots), bf16)]
    if absolute:
        outs.append(jax.ShapeDtypeStruct((hid_count, per_dest, n_wide), bf16))
    else:
        outs += [jax.ShapeDtypeStruct((per_dest, n_wide), bf16)] * hid_count
    n_in, n_out = len(operands) + 1, len(outs)

    def kernel(*refs):
        apply_kernel(
            len(pairs), sizes, unit_row, own_half, refs[:n_in], refs[n_in : n_in + n_out], refs[n_in + n_out :]
        )

    wide = (padded_pairs(k_count) + padded_pairs(n_count)) * PAIR
    whole = pl.BlockSpec(memory_space=VMEM)
    flops = 2 * slots * k_wide * n_wide
    return pl.pallas_call(
        kernel,
        in_specs=[whole] * len(operands) + [pl.BlockSpec(memory_space=pl.ANY)],
        out_specs=[whole] * n_out,
        out_shape=outs,
        scratch_shapes=[
            VMEM((chunks, k_wide, chunk), bf16),
            VMEM((320, 2 * LANES), bf16),
            VMEM((PIN, 2 * LANES), f32),
            VMEM((slots, wide), f32),
            VMEM((slots, k_wide), bf16),
            VMEM((slots, n_wide), bf16),
            VMEM((slots, n_wide), f32),
            pltpu.SemaphoreType.DMA((chunks,)),
        ],
        compiler_params=pltpu.CompilerParams(vmem_limit_bytes=58 << 20),
        cost_estimate=pl.CostEstimate(flops=flops, transcendentals=0, bytes_accessed=2 * k_wide * n_wide),
        name="apply_rows",
    )(*operands, curvature)


def update_kernel(factor, kt_ref, n_ref, c_ref, out_ref):
    gram = jnp.dot(kt_ref[...], n_ref[...], preferred_element_type=f32)
    out_ref[...] = (c_ref[...].astype(f32) + gram * factor).astype(bf16)


def update(rows_kt, rows_n, curvature, factor):
    k_wide, n_wide = curvature.shape
    slots = rows_n.shape[0]
    block = k_wide // 9
    return pl.pallas_call(
        functools.partial(update_kernel, factor),
        grid=(k_wide // block,),
        in_specs=[
            pl.BlockSpec((block, slots), lambda k: (k, 0)),
            pl.BlockSpec((slots, n_wide), lambda k: (0, 0)),
            pl.BlockSpec((block, n_wide), lambda k: (k, 0)),
        ],
        out_specs=pl.BlockSpec((block, n_wide), lambda k: (k, 0)),
        out_shape=jax.ShapeDtypeStruct(curvature.shape, bf16),
        compiler_params=pltpu.CompilerParams(dimension_semantics=("arbitrary",), vmem_limit_bytes=40 << 20),
        cost_estimate=pl.CostEstimate(
            flops=8 * slots * k_wide * n_wide, transcendentals=0, bytes_accessed=4 * k_wide * n_wide
        ),
        name="update",
    )(rows_kt, rows_n, curvature)


def summed(terms):
    total = terms[0].astype(f32)
    for term in terms[1:]:
        total = total + term.astype(f32)
    return total


def per_device(inputs, out_grads, proj_in, proj_out, curvature):
    hid_count, col_count = lax.axis_size("hid"), lax.axis_size("col")
    own = inputs.shape[0] // SEQ
    examples = own * col_count
    groups = hid_count // col_count
    each = own // groups
    assert groups * each == own and groups * col_count == hid_count
    per_dest = -(-each // SUB) * SUB
    lanes = groups * per_dest * SEQ
    slots = groups * per_dest * col_count
    factor = gram_weight / examples
    units = lanes // (2 * LANES)
    fast = lanes == hid_count * LANES and hid_count % 4 == 0 and col_count == 4

    if fast:
        pieces = project(inputs, out_grads, proj_in, proj_out, lanes, groups, hid_count)

        def over(axis, count, to):
            return lambda x: lax.ppermute(x, axis, [(i, to(i)) for i in range(count)])

        got = [pieces[0]]
        for d in range(1, hid_count):
            got.append(over("hid", hid_count, lambda i, d=d: i ^ d)(pieces[d]))
        piece = summed(got).astype(bf16)

        depth = hid_count // 2
        ring = [piece]
        for d in range(1, depth):
            ring.append(over("hid", hid_count, lambda i, d=d: (i + 2 * d) % hid_count)(piece))
        low, high = jnp.stack(ring[: depth // 2]), jnp.stack(ring[depth // 2 :])
        to_y = over("hid", hid_count, lambda i: i ^ 1)
        to_x = over("col", col_count, lambda i: i ^ 2)
        to_core = over("col", col_count, lambda i: i ^ 1)
        low_y, high_y = to_y(low), to_y(high)
        low_x, high_x = to_x(low), to_x(high)
        low_xy, high_xy = to_x(low_y), to_y(high_x)
        mine = [(low, low_y), (high, high_y), (low_x, low_xy), (high_x, high_xy)]
        theirs = [(to_core(a), to_core(b)) for a, b in mine]
        pairs = mine + theirs

        def unit_row(at, j):
            hid, col = lax.axis_index("hid"), lax.axis_index("col")
            flip = (2 if at % 4 >= 2 else 0) + (1 if at >= 4 else 0)
            shift = j + (depth // 2 if at % 2 else 0)
            z = lax.rem(hid // 2 - shift + depth, depth)
            return (col ^ flip) * units + z

        def own_half():
            return lax.rem(lax.axis_index("hid"), 2)
    else:
        (part,) = project(inputs, out_grads, proj_in, proj_out, lanes, groups, 1)
        whole = lax.all_gather(lax.psum(part, "hid").astype(bf16), "col", axis=0, tiled=False)
        split = whole.reshape(col_count, FEATURES, units, 2, LANES).transpose(3, 0, 2, 1, 4)
        split = split.reshape(2, col_count * units, FEATURES, LANES)
        pairs = [(split[0], split[1])]

        def unit_row(at, j):
            return j

        def own_half():
            return jnp.int32(0)

    rows_n, rows_kt, *applied = apply_rows(
        pairs, curvature, hid_count, slots, per_dest, factor, unit_row, own_half, not fast
    )
    if fast:
        got = [applied[0]]
        for d in range(1, hid_count):
            got.append(over("hid", hid_count, lambda i, d=d: i ^ d)(applied[d]))
    else:
        got = lax.all_to_all(applied[0], "hid", 0, 0)
        got = [got[d] for d in range(hid_count)]
    curvature_new = update(rows_kt, rows_n, curvature, factor)
    return summed(got)[:each], curvature_new


def solution(mesh):
    in_specs = (P("col", "hid"), P("col", "hid"), P(None, "hid"), P(None, "hid"), P("hid", "col"))
    out_specs = (P("hid", "col"), P("hid", "col"))
    return jax.shard_map(
        per_device, mesh=mesh, in_specs=in_specs, out_specs=out_specs, check_vma=False
    )
```

```python
import functools

import jax
import jax.numpy as jnp
from jax import lax
from jax.experimental import pallas as pl
from jax.experimental.pallas import tpu as pltpu
from jax.sharding import PartitionSpec as P

PIN = 96
POUT = 192
SEQ = 32
FEATURES = PIN + POUT
LANES = 128
PAIR = 2 * POUT
SUB = 16

gram_weight = 1.0 / 64.0
apply_weight = 1.0 / 16.0


f32 = jnp.float32
bf16 = jnp.bfloat16
CONTRACT_LAST = (((1,), (1,)), ((), ()))
VMEM = pltpu.VMEM


def chunk_of(width, parts):
    return width // parts if width % (parts * LANES) == 0 else width


def project_kernel(pieces, groups, blocks, x_ref, g_ref, pin_ref, pout_ref, *refs):
    outs, (acc, x, g, pin, pout, sems) = refs[:pieces], refs[pieces:]
    copies = [(pout_ref, pout)]
    copies += [(g_ref.at[pl.ds(row, size)], g.at[pl.ds(row, size)]) for row, size, _ in blocks]
    copies += [(pin_ref, pin)]
    copies += [(x_ref.at[pl.ds(row, size)], x.at[pl.ds(row, size)]) for row, size, _ in blocks]
    copies = [pltpu.make_async_copy(*pair, sems.at[i]) for i, pair in enumerate(copies)]
    for copy in copies:
        copy.start()
    span = acc.shape[1] // groups
    for q in range(groups):
        acc[:, (q + 1) * span - LANES : (q + 1) * span] = jnp.zeros((FEATURES, LANES), f32)
    waits = iter(copies)
    for left, right, at in ((pout, g, slice(0, POUT)), (pin, x, slice(POUT, FEATURES))):
        next(waits).wait()
        for row, size, lane in blocks:
            next(waits).wait()
            acc[at, lane : lane + size] = lax.dot_general(
                left[...], right[row : row + size], CONTRACT_LAST, preferred_element_type=f32
            )
    if pieces == 1:
        outs[0][...] = acc[...]
    else:
        me = lax.axis_index("hid")
        for d in range(pieces):
            start = pl.multiple_of((me ^ d) * LANES, LANES)
            outs[d][...] = acc[:, pl.ds(start, LANES)].astype(bf16)


def project(inputs, out_grads, proj_in, proj_out, lanes, groups, pieces):
    tokens = inputs.shape[0]
    size, span = tokens // groups, lanes // groups
    blocks = []
    for q in range(groups):
        for at in range(0, size, 256):
            blocks.append((q * size + at, min(256, size - at), q * span + at))
    out = (
        [jax.ShapeDtypeStruct((FEATURES, lanes), f32)]
        if pieces == 1
        else [jax.ShapeDtypeStruct((FEATURES, LANES), bf16)] * pieces
    )
    operands = (inputs, out_grads, proj_in, proj_out)
    return pl.pallas_call(
        functools.partial(project_kernel, pieces, groups, tuple(blocks)),
        in_specs=[pl.BlockSpec(memory_space=pltpu.HBM)] * 4,
        out_specs=[pl.BlockSpec(memory_space=VMEM)] * pieces,
        out_shape=out,
        scratch_shapes=[VMEM((FEATURES, lanes), f32)]
        + [VMEM(x.shape, bf16) for x in operands]
        + [pltpu.SemaphoreType.DMA((2 * len(blocks) + 2,))],
        compiler_params=pltpu.CompilerParams(vmem_limit_bytes=62 << 20),
        name="project",
    )(*operands)


def padded_pairs(count):
    return -(-count // 2)


def apply_kernel(parts, sizes, unit_row, own_half, refs_in, outs, scratch):
    k_count, n_count, factor, per_dest, absolute = sizes
    curv = refs_in[-1]
    rows_n_out, rows_kt_out, applied_outs = outs[0], outs[1], outs[2:]
    stage, feats, rows, rk, acc, sems = scratch
    chunks = stage.shape[0]
    chunk = stage.shape[2]

    def copy(j):
        return pltpu.make_async_copy(curv.at[:, pl.ds(j * chunk, chunk)], stage.at[j], sems.at[j])

    for j in range(chunks):
        copy(j).start()

    hid, col = lax.axis_index("hid"), lax.axis_index("col")
    half = own_half()
    lane = lax.broadcasted_iota(jnp.int32, (8, 2 * LANES), 1)
    sub = lax.broadcasted_iota(jnp.int32, (8, 2 * LANES), 0)
    side = (lane >= LANES).astype(jnp.int32)
    side = side + half - 2 * side * half
    belongs = sub == side * 4 + (lane % LANES) // SEQ
    mask = belongs.astype(f32)

    k_pairs, n_pairs = padded_pairs(k_count), padded_pairs(n_count)
    blank = jnp.zeros((64, 2 * LANES), bf16)

    def unit(a_ref, b_ref, j, row0, spot):
        a, b = a_ref[j], b_ref[j]
        feats[spot, :, :LANES] = a[POUT:].astype(f32)
        feats[spot, :, LANES:] = b[POUT:].astype(f32)
        grads = jnp.concatenate([a[:POUT], b[:POUT]], axis=1)

        def tall(base, count, odd):
            got = []
            for p in range(padded_pairs(count)):
                i = 2 * p + odd
                if i < count:
                    got.append(jnp.broadcast_to(feats[spot, pl.ds(base + i, 1), :], (8, 2 * LANES)) * mask)
                else:
                    got.append(jnp.zeros((8, 2 * LANES), f32))
            return got

        even = tall(hid * k_count, k_count, 0) + tall(col * n_count, n_count, 0)
        odd = tall(hid * k_count, k_count, 1) + tall(col * n_count, n_count, 1)
        even = jnp.concatenate(even, axis=0).astype(bf16)
        odd = jnp.concatenate(odd, axis=0).astype(bf16)
        after, before = jnp.concatenate([grads, blank], axis=0), jnp.concatenate([blank, grads], axis=0)
        left = lax.dot_general(even, after, CONTRACT_LAST, preferred_element_type=f32)
        right = lax.dot_general(odd, before, CONTRACT_LAST, preferred_element_type=f32)
        for p in range(k_pairs + n_pairs):
            le, ri = left[8 * p : 8 * p + 8], right[8 * p : 8 * p + 8]
            rows[pl.ds(row0, 8), PAIR * p : PAIR * p + LANES] = le[:, :LANES]
            rows[pl.ds(row0, 8), PAIR * p + LANES : PAIR * p + 2 * LANES] = le[:, LANES:] + ri[:, :LANES]
            rows[pl.ds(row0, 8), PAIR * p + 2 * LANES : PAIR * (p + 1)] = ri[:, LANES:]

    spots = feats.shape[0]
    for at in range(parts):
        a_ref, b_ref = refs_in[2 * at], refs_in[2 * at + 1]
        if absolute:

            @pl.loop(0, a_ref.shape[0])
            def _(j, at=at, a_ref=a_ref, b_ref=b_ref):
                unit(a_ref, b_ref, j, pl.multiple_of(8 * unit_row(at, j), 8), 0)
        else:
            for j in range(a_ref.shape[0]):
                spot = (at * a_ref.shape[0] + j) % spots
                unit(a_ref, b_ref, j, pl.multiple_of(8 * unit_row(at, j), 8), spot)

    k_wide, n_wide = k_count * POUT, n_count * POUT
    rk[...] = rows[:, :k_wide].astype(bf16)
    rn = rows_n_out
    rn[...] = rows[:, k_pairs * PAIR : k_pairs * PAIR + n_wide].astype(bf16)
    rows_kt_out[...] = rk[...].T

    inner = lax.dot_general(rk[...], rk[...], CONTRACT_LAST, preferred_element_type=f32) * factor
    high = inner.astype(bf16)
    low = (inner - high.astype(f32)).astype(bf16)

    both = jnp.concatenate([high, low], axis=1)
    step = 256 if chunk % 256 == 0 else chunk
    for j in range(chunks):
        copy(j).wait()
        for k in range(0, chunk, step):
            at = slice(j * chunk + k, j * chunk + k + step)
            near = rn[:, at]
            small = jnp.dot(both, jnp.concatenate([near, near], axis=0), preferred_element_type=f32)
            big = jnp.dot(rk[...], stage[j, :, k : k + step], preferred_element_type=f32)
            acc[:, at] = (big + small) * apply_weight

    if absolute:
        applied_outs[0][...] = acc[...].astype(bf16).reshape(applied_outs[0].shape)
    else:
        for d in range(len(applied_outs)):
            start = pl.multiple_of((hid ^ d) * per_dest, 8)
            applied_outs[d][...] = acc[pl.ds(start, per_dest), :].astype(bf16)


def apply_rows(pairs, curvature, hid_count, slots, per_dest, factor, unit_row, own_half, absolute):
    k_wide, n_wide = curvature.shape
    k_count, n_count = k_wide // POUT, n_wide // POUT
    chunk = chunk_of(n_wide, 9)
    chunks = n_wide // chunk
    operands = [x for pair in pairs for x in pair]
    sizes = (k_count, n_count, factor, per_dest, absolute)
    outs = [jax.ShapeDtypeStruct((slots, n_wide), bf16), jax.ShapeDtypeStruct((k_wide, slots), bf16)]
    if absolute:
        outs.append(jax.ShapeDtypeStruct((hid_count, per_dest, n_wide), bf16))
    else:
        outs += [jax.ShapeDtypeStruct((per_dest, n_wide), bf16)] * hid_count
    n_in, n_out = len(operands) + 1, len(outs)

    def kernel(*refs):
        apply_kernel(
            len(pairs), sizes, unit_row, own_half, refs[:n_in], refs[n_in : n_in + n_out], refs[n_in + n_out :]
        )

    wide = (padded_pairs(k_count) + padded_pairs(n_count)) * PAIR
    whole = pl.BlockSpec(memory_space=VMEM)
    flops = 2 * slots * k_wide * n_wide
    return pl.pallas_call(
        kernel,
        in_specs=[whole] * len(operands) + [pl.BlockSpec(memory_space=pltpu.HBM)],
        out_specs=[whole] * n_out,
        out_shape=outs,
        scratch_shapes=[
            VMEM((chunks, k_wide, chunk), bf16),
            VMEM((4, PIN, 2 * LANES), f32),
            VMEM((slots, wide), f32),
            VMEM((slots, k_wide), bf16),
            VMEM((slots, n_wide), f32),
            pltpu.SemaphoreType.DMA((chunks,)),
        ],
        compiler_params=pltpu.CompilerParams(vmem_limit_bytes=44 << 20),
        cost_estimate=pl.CostEstimate(flops=flops, transcendentals=0, bytes_accessed=2 * k_wide * n_wide),
        name="apply_rows",
    )(*operands, curvature)


def update_kernel(factor, kt_ref, n_ref, c_ref, out_ref, held, ins, outs):
    blocks, block, n_wide = held.shape
    step = 512 if n_wide % 512 == 0 else n_wide

    def read(j):
        return pltpu.make_async_copy(c_ref.at[pl.ds(j * block, block)], held.at[j], ins.at[j])

    def write(j):
        return pltpu.make_async_copy(held.at[j], out_ref.at[pl.ds(j * block, block)], outs.at[j])

    for j in range(blocks):
        read(j).start()

    @pl.loop(0, blocks)
    def _(j):
        read(j).wait()
        left = kt_ref[pl.ds(pl.multiple_of(j * block, block), block), :]
        for at in range(0, n_wide, step):
            gram = jnp.dot(left, n_ref[:, at : at + step], preferred_element_type=f32)
            old = held[j, :, at : at + step].astype(f32)
            held[j, :, at : at + step] = (old + gram * factor).astype(bf16)
        write(j).start()

    for j in range(blocks):
        write(j).wait()


def update(rows_kt, rows_n, curvature, factor):
    k_wide, n_wide = curvature.shape
    slots = rows_n.shape[0]
    blocks = 18
    whole = pl.BlockSpec(memory_space=VMEM)
    apart = pl.BlockSpec(memory_space=pltpu.HBM)
    return pl.pallas_call(
        functools.partial(update_kernel, factor),
        in_specs=[whole, whole, apart],
        out_specs=apart,
        out_shape=jax.ShapeDtypeStruct(curvature.shape, bf16),
        scratch_shapes=[
            VMEM((blocks, k_wide // blocks, n_wide), bf16),
            pltpu.SemaphoreType.DMA((blocks,)),
            pltpu.SemaphoreType.DMA((blocks,)),
        ],
        compiler_params=pltpu.CompilerParams(vmem_limit_bytes=40 << 20),
        cost_estimate=pl.CostEstimate(
            flops=8 * slots * k_wide * n_wide, transcendentals=0, bytes_accessed=4 * k_wide * n_wide
        ),
        name="update",
    )(rows_kt, rows_n, curvature)


def summed(terms):
    total = terms[0].astype(f32)
    for term in terms[1:]:
        total = total + term.astype(f32)
    return total


def per_device(inputs, out_grads, proj_in, proj_out, curvature):
    hid_count, col_count = lax.axis_size("hid"), lax.axis_size("col")
    own = inputs.shape[0] // SEQ
    examples = own * col_count
    groups = hid_count // col_count
    each = own // groups
    assert groups * each == own and groups * col_count == hid_count
    per_dest = -(-each // SUB) * SUB
    lanes = groups * per_dest * SEQ
    slots = groups * per_dest * col_count
    factor = gram_weight / examples
    units = lanes // (2 * LANES)
    fast = lanes == hid_count * LANES and hid_count % 4 == 0 and col_count == 4

    if fast:
        pieces = project(inputs, out_grads, proj_in, proj_out, lanes, groups, hid_count)

        def over(axis, count, to):
            return lambda x: lax.ppermute(x, axis, [(i, to(i)) for i in range(count)])

        far_first = sorted(range(1, hid_count), key=lambda d: (-(d // 4), d))
        got = [pieces[0]]
        for d in far_first:
            got.append(over("hid", hid_count, lambda i, d=d: i ^ d)(pieces[d]))
        piece = summed(got).astype(bf16)

        depth = hid_count // 2
        ring = [piece]
        for d in range(1, depth):
            ring.append(over("hid", hid_count, lambda i, d=d: (i + 2 * d) % hid_count)(piece))
        low, high = jnp.stack(ring[: depth // 2]), jnp.stack(ring[depth // 2 :])
        to_y = over("hid", hid_count, lambda i: i ^ 1)
        to_x = over("col", col_count, lambda i: i ^ 2)
        to_core = over("col", col_count, lambda i: i ^ 1)
        low_y, high_y = to_y(low), to_y(high)
        low_x, high_x = to_x(low), to_x(high)
        low_xy, high_xy = to_x(low_y), to_y(high_x)
        mine = [(low, low_y), (high, high_y), (low_x, low_xy), (high_x, high_xy)]
        theirs = [(to_core(a), to_core(b)) for a, b in mine]
        pairs = mine + theirs

        def unit_row(at, j):
            hid, col = lax.axis_index("hid"), lax.axis_index("col")
            flip = (2 if at % 4 >= 2 else 0) + (1 if at >= 4 else 0)
            shift = j + (depth // 2 if at % 2 else 0)
            z = lax.rem(hid // 2 - shift + depth, depth)
            return (col ^ flip) * units + z

        def own_half():
            return lax.rem(lax.axis_index("hid"), 2)
    else:
        (part,) = project(inputs, out_grads, proj_in, proj_out, lanes, groups, 1)
        whole = lax.all_gather(lax.psum(part, "hid").astype(bf16), "col", axis=0, tiled=False)
        split = whole.reshape(col_count, FEATURES, units, 2, LANES).transpose(3, 0, 2, 1, 4)
        split = split.reshape(2, col_count * units, FEATURES, LANES)
        pairs = [(split[0], split[1])]

        def unit_row(at, j):
            return j

        def own_half():
            return jnp.int32(0)

    rows_n, rows_kt, *applied = apply_rows(
        pairs, curvature, hid_count, slots, per_dest, factor, unit_row, own_half, not fast
    )
    if fast:
        got = [applied[0]]
        for d in far_first:
            got.append(over("hid", hid_count, lambda i, d=d: i ^ d)(applied[d]))
    else:
        got = lax.all_to_all(applied[0], "hid", 0, 0)
        got = [got[d] for d in range(hid_count)]
    curvature_new = update(rows_kt, rows_n, curvature, factor)
    return summed(got)[:each], curvature_new


def solution(mesh):
    in_specs = (P("col", "hid"), P("col", "hid"), P(None, "hid"), P(None, "hid"), P("hid", "col"))
    out_specs = (P("hid", "col"), P("hid", "col"))
    return jax.shard_map(
        per_device, mesh=mesh, in_specs=in_specs, out_specs=out_specs, check_vma=False
    )
```

```python
import functools

import jax
import jax.numpy as jnp
from jax import lax
from jax.experimental import pallas as pl
from jax.experimental.pallas import tpu as pltpu
from jax.sharding import PartitionSpec as P

PIN = 96
POUT = 192
SEQ = 32
FEATURES = PIN + POUT
LANES = 128
PAIR = 2 * POUT
SUB = 16

gram_weight = 1.0 / 64.0
apply_weight = 1.0 / 16.0


f32 = jnp.float32
bf16 = jnp.bfloat16
CONTRACT_LAST = (((1,), (1,)), ((), ()))
VMEM = pltpu.VMEM


def chunk_of(width, parts):
    return width // parts if width % (parts * LANES) == 0 else width


def project_kernel(pieces, groups, tokens, x_ref, g_ref, pin_ref, pout_ref, *refs):
    outs, (acc, x, g, pin, pout, sems) = refs[:pieces], refs[pieces:]
    span = acc.shape[1] // groups
    held = span // 256

    def part(which, i, k):
        source, target = ((g_ref, g), (x_ref, x))[which]
        at, size = k * 256, min(256, tokens - k * 256)
        sem = sems.at[2 + (which * groups + i) * held + k]
        return pltpu.make_async_copy(
            source.at[pl.ds(i * tokens + at, size)], target.at[pl.ds(i * span + at, size)], sem
        )

    weights = [pltpu.make_async_copy(pout_ref, pout, sems.at[0]), pltpu.make_async_copy(pin_ref, pin, sems.at[1])]
    for which in (0, 1):
        weights[which].start()
        for i in range(groups):
            for k in range(held):
                part(which, i, k).start()
    for which, left, right, at in ((0, pout, g, slice(0, POUT)), (1, pin, x, slice(POUT, FEATURES))):
        weights[which].wait()

        @pl.loop(0, groups * held)
        def _(j, which=which, left=left, right=right, at=at):
            for k in range(held):

                @pl.when(lax.rem(j, held) == k)
                def _(k=k):
                    part(which, j // held, k).wait()

            start = pl.multiple_of(j * 256, 256)
            acc[at, pl.ds(start, 256)] = lax.dot_general(
                left[...], right[pl.ds(start, 256)], CONTRACT_LAST, preferred_element_type=f32
            )
    lane = lax.broadcasted_iota(jnp.int32, (FEATURES, LANES), 1)
    for q in range(groups):
        last = slice((q + 1) * span - LANES, (q + 1) * span)
        acc[:, last] = jnp.where(lane < tokens - span + LANES, acc[:, last], 0.0)
    if pieces == 1:
        outs[0][...] = acc[...]
    else:
        me = lax.axis_index("hid")
        for d in range(pieces):
            start = pl.multiple_of((me ^ d) * LANES, LANES)
            outs[d][...] = acc[:, pl.ds(start, LANES)].astype(bf16)


def project(inputs, out_grads, proj_in, proj_out, lanes, groups, pieces):
    tokens = inputs.shape[0]
    size, span = tokens // groups, lanes // groups
    out = (
        [jax.ShapeDtypeStruct((FEATURES, lanes), f32)]
        if pieces == 1
        else [jax.ShapeDtypeStruct((FEATURES, LANES), bf16)] * pieces
    )
    operands = (inputs, out_grads, proj_in, proj_out)
    return pl.pallas_call(
        functools.partial(project_kernel, pieces, groups, size),
        in_specs=[pl.BlockSpec(memory_space=pltpu.HBM)] * 4,
        out_specs=[pl.BlockSpec(memory_space=VMEM)] * pieces,
        out_shape=out,
        scratch_shapes=[VMEM((FEATURES, lanes), f32)]
        + [VMEM((lanes, x.shape[1]), bf16) for x in operands[:2]]
        + [VMEM(x.shape, bf16) for x in operands[2:]]
        + [pltpu.SemaphoreType.DMA((2 * groups * (span // 256) + 2,))],
        compiler_params=pltpu.CompilerParams(vmem_limit_bytes=62 << 20),
        name="project",
    )(*operands)


def padded_pairs(count):
    return -(-count // 2)


def apply_kernel(parts, sizes, unit_row, own_half, refs_in, outs, scratch):
    k_count, n_count, factor, per_dest, absolute = sizes
    curv = refs_in[-1]
    rows_n_out, rows_kt_out, applied_outs = outs[0], outs[1], outs[2:]
    stage, feats, rows, rk, both, acc, sems = scratch
    chunks = stage.shape[0]
    chunk = stage.shape[2]

    def copy(j):
        return pltpu.make_async_copy(curv.at[:, pl.ds(j * chunk, chunk)], stage.at[j], sems.at[j])

    for j in range(chunks):
        copy(j).start()

    hid, col = lax.axis_index("hid"), lax.axis_index("col")
    half = own_half()
    lane = lax.broadcasted_iota(jnp.int32, (8, 2 * LANES), 1)
    sub = lax.broadcasted_iota(jnp.int32, (8, 2 * LANES), 0)
    side = (lane >= LANES).astype(jnp.int32)
    side = side + half - 2 * side * half
    belongs = sub == side * 4 + (lane % LANES) // SEQ
    mask = belongs.astype(f32)

    k_pairs, n_pairs = padded_pairs(k_count), padded_pairs(n_count)
    blank = jnp.zeros((64, 2 * LANES), bf16)

    def unit(a_ref, b_ref, j, row0, spot):
        a, b = a_ref[j], b_ref[j]
        feats[spot, :, :LANES] = a[POUT:].astype(f32)
        feats[spot, :, LANES:] = b[POUT:].astype(f32)
        grads = jnp.concatenate([a[:POUT], b[:POUT]], axis=1)

        def tall(base, count, odd):
            got = []
            for p in range(padded_pairs(count)):
                i = 2 * p + odd
                if i < count:
                    got.append(jnp.broadcast_to(feats[spot, pl.ds(base + i, 1), :], (8, 2 * LANES)) * mask)
                else:
                    got.append(jnp.zeros((8, 2 * LANES), f32))
            return got

        even = tall(hid * k_count, k_count, 0) + tall(col * n_count, n_count, 0)
        odd = tall(hid * k_count, k_count, 1) + tall(col * n_count, n_count, 1)
        even = jnp.concatenate(even, axis=0).astype(bf16)
        odd = jnp.concatenate(odd, axis=0).astype(bf16)
        after, before = jnp.concatenate([grads, blank], axis=0), jnp.concatenate([blank, grads], axis=0)
        left = lax.dot_general(even, after, CONTRACT_LAST, preferred_element_type=f32)
        right = lax.dot_general(odd, before, CONTRACT_LAST, preferred_element_type=f32)
        for p in range(k_pairs + n_pairs):
            le, ri = left[8 * p : 8 * p + 8], right[8 * p : 8 * p + 8]
            rows[pl.ds(row0, 8), PAIR * p : PAIR * p + LANES] = le[:, :LANES]
            rows[pl.ds(row0, 8), PAIR * p + LANES : PAIR * p + 2 * LANES] = le[:, LANES:] + ri[:, :LANES]
            rows[pl.ds(row0, 8), PAIR * p + 2 * LANES : PAIR * (p + 1)] = ri[:, LANES:]

    spots = feats.shape[0]
    for at in range(parts):
        a_ref, b_ref = refs_in[2 * at], refs_in[2 * at + 1]
        if absolute:

            @pl.loop(0, a_ref.shape[0])
            def _(j, at=at, a_ref=a_ref, b_ref=b_ref):
                unit(a_ref, b_ref, j, pl.multiple_of(8 * unit_row(at, j), 8), 0)
        else:
            for j in range(a_ref.shape[0]):
                spot = (at * a_ref.shape[0] + j) % spots
                unit(a_ref, b_ref, j, pl.multiple_of(8 * unit_row(at, j), 8), spot)

    k_wide, n_wide = k_count * POUT, n_count * POUT
    rk[...] = rows[:, :k_wide].astype(bf16)
    rn = rows_n_out
    rn[...] = rows[:, k_pairs * PAIR : k_pairs * PAIR + n_wide].astype(bf16)
    rows_kt_out[...] = rk[...].T

    inner = lax.dot_general(rk[...], rk[...], CONTRACT_LAST, preferred_element_type=f32) * factor
    high = inner.astype(bf16)
    low = (inner - high.astype(f32)).astype(bf16)

    slots = both.shape[0]
    both[:, :slots] = high
    both[:, slots:] = low
    step = 256 if chunk % 256 == 0 else chunk

    @pl.loop(0, chunks)
    def _(j):
        copy(j).wait()
        for k in range(0, chunk, step):
            at = pl.ds(pl.multiple_of(j * chunk + k, step), step)
            near = rn[:, at]
            small = jnp.dot(both[...], jnp.concatenate([near, near], axis=0), preferred_element_type=f32)
            big = jnp.dot(rk[...], stage[j, :, k : k + step], preferred_element_type=f32)
            acc[:, at] = (big + small) * apply_weight

    if absolute:
        applied_outs[0][...] = acc[...].astype(bf16).reshape(applied_outs[0].shape)
    else:
        for d in range(len(applied_outs)):
            start = pl.multiple_of((hid ^ d) * per_dest, 8)
            applied_outs[d][...] = acc[pl.ds(start, per_dest), :].astype(bf16)


def apply_rows(pairs, curvature, hid_count, slots, per_dest, factor, unit_row, own_half, absolute):
    k_wide, n_wide = curvature.shape
    k_count, n_count = k_wide // POUT, n_wide // POUT
    chunk = chunk_of(n_wide, 9)
    chunks = n_wide // chunk
    operands = [x for pair in pairs for x in pair]
    sizes = (k_count, n_count, factor, per_dest, absolute)
    outs = [jax.ShapeDtypeStruct((slots, n_wide), bf16), jax.ShapeDtypeStruct((k_wide, slots), bf16)]
    if absolute:
        outs.append(jax.ShapeDtypeStruct((hid_count, per_dest, n_wide), bf16))
    else:
        outs += [jax.ShapeDtypeStruct((per_dest, n_wide), bf16)] * hid_count
    n_in, n_out = len(operands) + 1, len(outs)

    def kernel(*refs):
        apply_kernel(
            len(pairs), sizes, unit_row, own_half, refs[:n_in], refs[n_in : n_in + n_out], refs[n_in + n_out :]
        )

    wide = (padded_pairs(k_count) + padded_pairs(n_count)) * PAIR
    whole = pl.BlockSpec(memory_space=VMEM)
    flops = 2 * slots * k_wide * n_wide
    return pl.pallas_call(
        kernel,
        in_specs=[whole] * len(operands) + [pl.BlockSpec(memory_space=pltpu.HBM)],
        out_specs=[whole] * n_out,
        out_shape=outs,
        scratch_shapes=[
            VMEM((chunks, k_wide, chunk), bf16),
            VMEM((4, PIN, 2 * LANES), f32),
            VMEM((slots, wide), f32),
            VMEM((slots, k_wide), bf16),
            VMEM((slots, 2 * slots), bf16),
            VMEM((slots, n_wide), f32),
            pltpu.SemaphoreType.DMA((chunks,)),
        ],
        compiler_params=pltpu.CompilerParams(vmem_limit_bytes=44 << 20),
        cost_estimate=pl.CostEstimate(flops=flops, transcendentals=0, bytes_accessed=2 * k_wide * n_wide),
        name="apply_rows",
    )(*operands, curvature)


def update_kernel(factor, kt_ref, n_ref, c_ref, out_ref, held, ins, outs):
    blocks, block, n_wide = held.shape
    step = 512 if n_wide % 512 == 0 else n_wide

    def read(j):
        return pltpu.make_async_copy(c_ref.at[pl.ds(j * block, block)], held.at[j], ins.at[j])

    def write(j):
        return pltpu.make_async_copy(held.at[j], out_ref.at[pl.ds(j * block, block)], outs.at[j])

    ahead = min(10, blocks)
    for j in range(ahead):
        read(j).start()

    @pl.loop(0, blocks)
    def _(j):
        read(j).wait()

        @pl.when(j + ahead < blocks)
        def _():
            read(j + ahead).start()

        left = kt_ref[pl.ds(pl.multiple_of(j * block, block), block), :]
        for at in range(0, n_wide, step):
            gram = jnp.dot(left, n_ref[:, at : at + step], preferred_element_type=f32)
            old = held[j, :, at : at + step].astype(f32)
            held[j, :, at : at + step] = (old + gram * factor).astype(bf16)
        write(j).start()

    for j in range(blocks):
        write(j).wait()


def update(rows_kt, rows_n, curvature, factor):
    k_wide, n_wide = curvature.shape
    slots = rows_n.shape[0]
    blocks = 18
    whole = pl.BlockSpec(memory_space=VMEM)
    apart = pl.BlockSpec(memory_space=pltpu.HBM)
    return pl.pallas_call(
        functools.partial(update_kernel, factor),
        in_specs=[whole, whole, apart],
        out_specs=apart,
        out_shape=jax.ShapeDtypeStruct(curvature.shape, bf16),
        scratch_shapes=[
            VMEM((blocks, k_wide // blocks, n_wide), bf16),
            pltpu.SemaphoreType.DMA((blocks,)),
            pltpu.SemaphoreType.DMA((blocks,)),
        ],
        compiler_params=pltpu.CompilerParams(vmem_limit_bytes=40 << 20),
        cost_estimate=pl.CostEstimate(
            flops=8 * slots * k_wide * n_wide, transcendentals=0, bytes_accessed=4 * k_wide * n_wide
        ),
        name="update",
    )(rows_kt, rows_n, curvature)


def summed(terms):
    total = terms[0].astype(f32)
    for term in terms[1:]:
        total = total + term.astype(f32)
    return total


def per_device(inputs, out_grads, proj_in, proj_out, curvature):
    hid_count, col_count = lax.axis_size("hid"), lax.axis_size("col")
    own = inputs.shape[0] // SEQ
    examples = own * col_count
    groups = hid_count // col_count
    each = own // groups
    assert groups * each == own and groups * col_count == hid_count
    per_dest = -(-each // SUB) * SUB
    lanes = groups * per_dest * SEQ
    slots = groups * per_dest * col_count
    factor = gram_weight / examples
    units = lanes // (2 * LANES)
    fast = lanes == hid_count * LANES and hid_count % 4 == 0 and col_count == 4

    if fast:
        pieces = project(inputs, out_grads, proj_in, proj_out, lanes, groups, hid_count)

        def over(axis, count, to):
            return lambda x: lax.ppermute(x, axis, [(i, to(i)) for i in range(count)])

        far_first = sorted(range(1, hid_count), key=lambda d: (-(d // 4), d))
        got = [pieces[0]]
        for d in far_first:
            got.append(over("hid", hid_count, lambda i, d=d: i ^ d)(pieces[d]))
        piece = summed(got).astype(bf16)

        depth = hid_count // 2
        ring = [piece]
        for d in range(1, depth):
            ring.append(over("hid", hid_count, lambda i, d=d: (i + 2 * d) % hid_count)(piece))
        low, high = jnp.stack(ring[: depth // 2]), jnp.stack(ring[depth // 2 :])
        to_y = over("hid", hid_count, lambda i: i ^ 1)
        to_x = over("col", col_count, lambda i: i ^ 2)
        to_core = over("col", col_count, lambda i: i ^ 1)
        low_y, high_y = to_y(low), to_y(high)
        low_x, high_x = to_x(low), to_x(high)
        low_xy, high_xy = to_x(low_y), to_y(high_x)
        mine = [(low, low_y), (high, high_y), (low_x, low_xy), (high_x, high_xy)]
        theirs = [(to_core(a), to_core(b)) for a, b in mine]
        pairs = mine + theirs

        def unit_row(at, j):
            hid, col = lax.axis_index("hid"), lax.axis_index("col")
            flip = (2 if at % 4 >= 2 else 0) + (1 if at >= 4 else 0)
            shift = j + (depth // 2 if at % 2 else 0)
            z = lax.rem(hid // 2 - shift + depth, depth)
            return (col ^ flip) * units + z

        def own_half():
            return lax.rem(lax.axis_index("hid"), 2)
    else:
        (part,) = project(inputs, out_grads, proj_in, proj_out, lanes, groups, 1)
        whole = lax.all_gather(lax.psum(part, "hid").astype(bf16), "col", axis=0, tiled=False)
        split = whole.reshape(col_count, FEATURES, units, 2, LANES).transpose(3, 0, 2, 1, 4)
        split = split.reshape(2, col_count * units, FEATURES, LANES)
        pairs = [(split[0], split[1])]

        def unit_row(at, j):
            return j

        def own_half():
            return jnp.int32(0)

    rows_n, rows_kt, *applied = apply_rows(
        pairs, curvature, hid_count, slots, per_dest, factor, unit_row, own_half, not fast
    )
    if fast:
        got = [applied[0]]
        for d in far_first:
            got.append(over("hid", hid_count, lambda i, d=d: i ^ d)(applied[d]))
    else:
        got = lax.all_to_all(applied[0], "hid", 0, 0)
        got = [got[d] for d in range(hid_count)]
    curvature_new = update(rows_kt, rows_n, curvature, factor)
    return summed(got)[:each], curvature_new


def solution(mesh):
    in_specs = (P("col", "hid"), P("col", "hid"), P(None, "hid"), P(None, "hid"), P("hid", "col"))
    out_specs = (P("hid", "col"), P("hid", "col"))
    return jax.shard_map(
        per_device, mesh=mesh, in_specs=in_specs, out_specs=out_specs, check_vma=False
    )
```

```python
import functools

import jax
import jax.numpy as jnp
from jax import lax
from jax.experimental import pallas as pl
from jax.experimental.pallas import tpu as pltpu
from jax.sharding import PartitionSpec as P

PIN = 96
POUT = 192
SEQ = 32
FEATURES = PIN + POUT
LANES = 128
PAIR = 2 * POUT
SUB = 16
NEAR = 4

gram_weight = 1.0 / 64.0
apply_weight = 1.0 / 16.0


f32 = jnp.float32
bf16 = jnp.bfloat16
CONTRACT_LAST = (((1,), (1,)), ((), ()))
VMEM = pltpu.VMEM


def chunk_of(width, parts):
    return width // parts if width % (parts * LANES) == 0 else width


def project_kernel(pieces, groups, tokens, x_ref, g_ref, pin_ref, pout_ref, *refs):
    outs, (acc, x, g, pin, pout, sems) = refs[:pieces], refs[pieces:]
    span = acc.shape[1] // groups
    held = span // 256

    def part(which, i, k):
        source, target = ((g_ref, g), (x_ref, x))[which]
        at, size = k * 256, min(256, tokens - k * 256)
        sem = sems.at[2 + (which * groups + i) * held + k]
        return pltpu.make_async_copy(
            source.at[pl.ds(i * tokens + at, size)], target.at[pl.ds(i * span + at, size)], sem
        )

    weights = [pltpu.make_async_copy(pout_ref, pout, sems.at[0]), pltpu.make_async_copy(pin_ref, pin, sems.at[1])]
    for which in (0, 1):
        weights[which].start()
        for i in range(groups):
            for k in range(held):
                part(which, i, k).start()
    for which, left, right, at in ((0, pout, g, slice(0, POUT)), (1, pin, x, slice(POUT, FEATURES))):
        weights[which].wait()

        @pl.loop(0, groups * held)
        def _(j, which=which, left=left, right=right, at=at):
            for k in range(held):

                @pl.when(lax.rem(j, held) == k)
                def _(k=k):
                    part(which, j // held, k).wait()

            start = pl.multiple_of(j * 256, 256)
            acc[at, pl.ds(start, 256)] = lax.dot_general(
                left[...], right[pl.ds(start, 256)], CONTRACT_LAST, preferred_element_type=f32
            )
    lane = lax.broadcasted_iota(jnp.int32, (FEATURES, LANES), 1)
    for q in range(groups):
        last = slice((q + 1) * span - LANES, (q + 1) * span)
        acc[:, last] = jnp.where(lane < tokens - span + LANES, acc[:, last], 0.0)
    if pieces == 1:
        outs[0][...] = acc[...]
    else:
        me = lax.axis_index("hid")
        for d in range(pieces):
            start = pl.multiple_of((me ^ d) * LANES, LANES)
            outs[d][...] = acc[:, pl.ds(start, LANES)].astype(bf16)


def project(inputs, out_grads, proj_in, proj_out, lanes, groups, pieces):
    tokens = inputs.shape[0]
    size, span = tokens // groups, lanes // groups
    out = (
        [jax.ShapeDtypeStruct((FEATURES, lanes), f32)]
        if pieces == 1
        else [jax.ShapeDtypeStruct((FEATURES, LANES), bf16)] * pieces
    )
    operands = (inputs, out_grads, proj_in, proj_out)
    return pl.pallas_call(
        functools.partial(project_kernel, pieces, groups, size),
        in_specs=[pl.BlockSpec(memory_space=pltpu.HBM)] * 4,
        out_specs=[pl.BlockSpec(memory_space=VMEM)] * pieces,
        out_shape=out,
        scratch_shapes=[VMEM((FEATURES, lanes), f32)]
        + [VMEM((lanes, x.shape[1]), bf16) for x in operands[:2]]
        + [VMEM(x.shape, bf16) for x in operands[2:]]
        + [pltpu.SemaphoreType.DMA((2 * groups * (span // 256) + 2,))],
        compiler_params=pltpu.CompilerParams(vmem_limit_bytes=62 << 20),
        name="project",
    )(*operands)


def padded_pairs(count):
    return -(-count // 2)


def apply_kernel(parts, sizes, unit_row, own_half, refs_in, outs, scratch):
    k_count, n_count, factor, per_dest, absolute = sizes
    curv = refs_in[-1]
    rows_n_out, rows_kt_out, stage, applied_outs = outs[0], outs[1], outs[2], outs[3:]
    feats, rows, rk, both, acc, sems = scratch
    chunks = stage.shape[0]
    chunk = stage.shape[2]

    def copy(j):
        return pltpu.make_async_copy(curv.at[:, pl.ds(j * chunk, chunk)], stage.at[j], sems.at[j])

    for j in range(chunks):
        copy(j).start()

    hid, col = lax.axis_index("hid"), lax.axis_index("col")
    half = own_half()
    lane = lax.broadcasted_iota(jnp.int32, (8, 2 * LANES), 1)
    sub = lax.broadcasted_iota(jnp.int32, (8, 2 * LANES), 0)
    side = (lane >= LANES).astype(jnp.int32)
    side = side + half - 2 * side * half
    belongs = sub == side * 4 + (lane % LANES) // SEQ
    mask = belongs.astype(f32)

    k_pairs, n_pairs = padded_pairs(k_count), padded_pairs(n_count)
    blank = jnp.zeros((64, 2 * LANES), bf16)

    def unit(a_ref, b_ref, j, row0, spot):
        a, b = a_ref[j], b_ref[j]
        feats[spot, :, :LANES] = a[POUT:].astype(f32)
        feats[spot, :, LANES:] = b[POUT:].astype(f32)
        grads = jnp.concatenate([a[:POUT], b[:POUT]], axis=1)

        def tall(base, count, odd):
            got = []
            for p in range(padded_pairs(count)):
                i = 2 * p + odd
                if i < count:
                    got.append(jnp.broadcast_to(feats[spot, pl.ds(base + i, 1), :], (8, 2 * LANES)) * mask)
                else:
                    got.append(jnp.zeros((8, 2 * LANES), f32))
            return got

        even = tall(hid * k_count, k_count, 0) + tall(col * n_count, n_count, 0)
        odd = tall(hid * k_count, k_count, 1) + tall(col * n_count, n_count, 1)
        even = jnp.concatenate(even, axis=0).astype(bf16)
        odd = jnp.concatenate(odd, axis=0).astype(bf16)
        after, before = jnp.concatenate([grads, blank], axis=0), jnp.concatenate([blank, grads], axis=0)
        left = lax.dot_general(even, after, CONTRACT_LAST, preferred_element_type=f32)
        right = lax.dot_general(odd, before, CONTRACT_LAST, preferred_element_type=f32)
        for p in range(k_pairs + n_pairs):
            le, ri = left[8 * p : 8 * p + 8], right[8 * p : 8 * p + 8]
            rows[pl.ds(row0, 8), PAIR * p : PAIR * p + LANES] = le[:, :LANES]
            rows[pl.ds(row0, 8), PAIR * p + LANES : PAIR * p + 2 * LANES] = le[:, LANES:] + ri[:, :LANES]
            rows[pl.ds(row0, 8), PAIR * p + 2 * LANES : PAIR * (p + 1)] = ri[:, LANES:]

    spots = feats.shape[0]
    for at in range(parts):
        a_ref, b_ref = refs_in[2 * at], refs_in[2 * at + 1]
        if absolute:

            @pl.loop(0, a_ref.shape[0])
            def _(j, at=at, a_ref=a_ref, b_ref=b_ref):
                unit(a_ref, b_ref, j, pl.multiple_of(8 * unit_row(at, j), 8), 0)
        else:
            for j in range(a_ref.shape[0]):
                spot = (at * a_ref.shape[0] + j) % spots
                unit(a_ref, b_ref, j, pl.multiple_of(8 * unit_row(at, j), 8), spot)

    k_wide, n_wide = k_count * POUT, n_count * POUT
    rk[...] = rows[:, :k_wide].astype(bf16)
    rn = rows_n_out
    rn[...] = rows[:, k_pairs * PAIR : k_pairs * PAIR + n_wide].astype(bf16)
    rows_kt_out[...] = rk[...].T

    inner = lax.dot_general(rk[...], rk[...], CONTRACT_LAST, preferred_element_type=f32) * factor
    high = inner.astype(bf16)
    low = (inner - high.astype(f32)).astype(bf16)

    slots = both.shape[0]
    both[:, :slots] = high
    both[:, slots:] = low
    step = 256 if chunk % 256 == 0 else chunk

    @pl.loop(0, chunks)
    def _(j):
        copy(j).wait()
        for k in range(0, chunk, step):
            at = pl.ds(pl.multiple_of(j * chunk + k, step), step)
            near = rn[:, at]
            small = jnp.dot(both[...], jnp.concatenate([near, near], axis=0), preferred_element_type=f32)
            big = jnp.dot(rk[...], stage[j, :, k : k + step], preferred_element_type=f32)
            acc[:, at] = (big + small) * apply_weight

    if absolute:
        applied_outs[0][...] = acc[...].astype(bf16).reshape(applied_outs[0].shape)
    else:
        for d, out in enumerate(applied_outs[:NEAR]):
            start = pl.multiple_of((hid ^ d) * per_dest, 8)
            out[...] = acc[pl.ds(start, per_dest), :].astype(bf16)
        at = 0
        for pair in zip(applied_outs[NEAR::2], applied_outs[NEAR + 1 :: 2]):
            for odd, out in enumerate(pair):
                for i in range(NEAR // 2):
                    start = pl.multiple_of((hid ^ (NEAR + 2 * i + odd)) * per_dest, 8)
                    out[i] = acc[pl.ds(start, per_dest), at : at + out.shape[-1]].astype(bf16)
            at += pair[0].shape[-1]


def apply_rows(pairs, curvature, hid_count, slots, per_dest, factor, unit_row, own_half, absolute):
    k_wide, n_wide = curvature.shape
    k_count, n_count = k_wide // POUT, n_wide // POUT
    chunk = chunk_of(n_wide, 9)
    chunks = n_wide // chunk
    operands = [x for pair in pairs for x in pair]
    sizes = (k_count, n_count, factor, per_dest, absolute)
    outs = [jax.ShapeDtypeStruct((slots, n_wide), bf16), jax.ShapeDtypeStruct((k_wide, slots), bf16)]
    outs.append(VMEM((chunks, k_wide, chunk), bf16))
    if absolute:
        outs.append(jax.ShapeDtypeStruct((hid_count, per_dest, n_wide), bf16))
    else:
        first = chunks // 2 * chunk
        outs += [jax.ShapeDtypeStruct((per_dest, n_wide), bf16)] * NEAR
        for part in (first, n_wide - first):
            outs += [jax.ShapeDtypeStruct((NEAR // 2, per_dest, part), bf16)] * 2
    n_in, n_out = len(operands) + 1, len(outs)

    def kernel(*refs):
        apply_kernel(
            len(pairs), sizes, unit_row, own_half, refs[:n_in], refs[n_in : n_in + n_out], refs[n_in + n_out :]
        )

    wide = (padded_pairs(k_count) + padded_pairs(n_count)) * PAIR
    whole = pl.BlockSpec(memory_space=VMEM)
    flops = 2 * slots * k_wide * n_wide
    return pl.pallas_call(
        kernel,
        in_specs=[whole] * len(operands) + [pl.BlockSpec(memory_space=pltpu.HBM)],
        out_specs=[whole] * n_out,
        out_shape=outs,
        scratch_shapes=[
            VMEM((4, PIN, 2 * LANES), f32),
            VMEM((slots, wide), f32),
            VMEM((slots, k_wide), bf16),
            VMEM((slots, 2 * slots), bf16),
            VMEM((slots, n_wide), f32),
            pltpu.SemaphoreType.DMA((chunks,)),
        ],
        compiler_params=pltpu.CompilerParams(vmem_limit_bytes=20 << 20),
        cost_estimate=pl.CostEstimate(flops=flops, transcendentals=0, bytes_accessed=2 * k_wide * n_wide),
        name="apply_rows",
    )(*operands, curvature)


def update_kernel(factor, low, high, kt_ref, n_ref, c_ref, *refs):
    out_ref, ready, sems = refs[-3:]
    _, k_wide, chunk = c_ref.shape
    slots = ready.shape[0]
    block = k_wide // 9

    def write(j):
        slot = lax.rem(j, slots)
        return pltpu.make_async_copy(ready.at[slot], out_ref.at[:, pl.ds(j * chunk, chunk)], sems.at[slot])

    @pl.loop(low, high)
    def _(j):
        @pl.when(j >= low + slots)
        def _():
            write(j - slots).wait()

        right = n_ref[:, pl.ds(pl.multiple_of(j * chunk, chunk), chunk)]
        slot = lax.rem(j, slots)
        for at in range(0, k_wide, block):
            gram = jnp.dot(kt_ref[at : at + block], right, preferred_element_type=f32)
            old = c_ref[j, at : at + block].astype(f32)
            ready[slot, at : at + block] = (old + gram * factor).astype(bf16)
        write(j).start()

    for j in range(high - slots, high):
        write(j).wait()


def update(rows_kt, rows_n, held, shape, factor, low, high, into=None):
    k_wide, n_wide = shape
    count = rows_n.shape[0]
    slots = min(4, high - low)
    more = [] if into is None else [into]
    share = (high - low) / held.shape[0]
    whole = pl.BlockSpec(memory_space=VMEM)
    return pl.pallas_call(
        functools.partial(update_kernel, factor, low, high),
        in_specs=[whole, whole, whole] + [pl.BlockSpec(memory_space=pltpu.HBM)] * len(more),
        input_output_aliases={3: 0} if more else {},
        out_specs=pl.BlockSpec(memory_space=pltpu.HBM),
        out_shape=jax.ShapeDtypeStruct(shape, bf16),
        scratch_shapes=[VMEM((slots,) + held.shape[1:], bf16), pltpu.SemaphoreType.DMA((slots,))],
        compiler_params=pltpu.CompilerParams(vmem_limit_bytes=16 << 20),
        cost_estimate=pl.CostEstimate(
            flops=int(8 * count * k_wide * n_wide * share),
            transcendentals=0,
            bytes_accessed=int(2 * k_wide * n_wide * share),
        ),
        name="update",
    )(rows_kt, rows_n, held, *more)


def join_kernel(own_ref, other_ref, *outs):
    for i, out in enumerate(outs):
        out[...] = (own_ref[i].astype(f32) + other_ref[i].astype(f32)).astype(bf16)


def join(own, other):
    count = own.shape[0]
    whole = pl.BlockSpec(memory_space=VMEM)
    return pl.pallas_call(
        join_kernel,
        in_specs=[whole, whole],
        out_specs=[whole] * count,
        out_shape=[jax.ShapeDtypeStruct(own.shape[1:], bf16)] * count,
        compiler_params=pltpu.CompilerParams(vmem_limit_bytes=4 << 20),
        name="join",
    )(own, other)


def summed(terms):
    total = terms[0].astype(f32)
    for term in terms[1:]:
        total = total + term.astype(f32)
    return total


def per_device(inputs, out_grads, proj_in, proj_out, curvature):
    hid_count, col_count = lax.axis_size("hid"), lax.axis_size("col")
    own = inputs.shape[0] // SEQ
    examples = own * col_count
    groups = hid_count // col_count
    each = own // groups
    assert groups * each == own and groups * col_count == hid_count
    per_dest = -(-each // SUB) * SUB
    lanes = groups * per_dest * SEQ
    slots = groups * per_dest * col_count
    factor = gram_weight / examples
    units = lanes // (2 * LANES)
    fast = lanes == hid_count * LANES and hid_count == 2 * NEAR and col_count == 4

    if fast:
        pieces = project(inputs, out_grads, proj_in, proj_out, lanes, groups, hid_count)

        def over(axis, count, to):
            return lambda x: lax.ppermute(x, axis, [(i, to(i)) for i in range(count)])

        far_first = sorted(range(1, hid_count), key=lambda d: (-(d // 4), d))
        got = [pieces[0]]
        for d in far_first:
            got.append(over("hid", hid_count, lambda i, d=d: i ^ d)(pieces[d]))
        piece = summed(got).astype(bf16)

        depth = hid_count // 2
        ring = [piece]
        for d in range(1, depth):
            ring.append(over("hid", hid_count, lambda i, d=d: (i + 2 * d) % hid_count)(piece))
        low, high = jnp.stack(ring[: depth // 2]), jnp.stack(ring[depth // 2 :])
        to_y = over("hid", hid_count, lambda i: i ^ 1)
        to_x = over("col", col_count, lambda i: i ^ 2)
        to_core = over("col", col_count, lambda i: i ^ 1)
        low_y, high_y = to_y(low), to_y(high)
        low_x, high_x = to_x(low), to_x(high)
        low_xy, high_xy = to_x(low_y), to_y(high_x)
        mine = [(low, low_y), (high, high_y), (low_x, low_xy), (high_x, high_xy)]
        theirs = [(to_core(a), to_core(b)) for a, b in mine]
        pairs = mine + theirs

        def unit_row(at, j):
            hid, col = lax.axis_index("hid"), lax.axis_index("col")
            flip = (2 if at % 4 >= 2 else 0) + (1 if at >= 4 else 0)
            shift = j + (depth // 2 if at % 2 else 0)
            z = lax.rem(hid // 2 - shift + depth, depth)
            return (col ^ flip) * units + z

        def own_half():
            return lax.rem(lax.axis_index("hid"), 2)
    else:
        (part,) = project(inputs, out_grads, proj_in, proj_out, lanes, groups, 1)
        whole = lax.all_gather(lax.psum(part, "hid").astype(bf16), "col", axis=0, tiled=False)
        split = whole.reshape(col_count, FEATURES, units, 2, LANES).transpose(3, 0, 2, 1, 4)
        split = split.reshape(2, col_count * units, FEATURES, LANES)
        pairs = [(split[0], split[1])]

        def unit_row(at, j):
            return j

        def own_half():
            return jnp.int32(0)

    rows_n, rows_kt, held, *applied = apply_rows(
        pairs, curvature, hid_count, slots, per_dest, factor, unit_row, own_half, not fast
    )
    middle = (held.shape[0] + 2) // 2
    curvature_new = update(rows_kt, rows_n, held, curvature.shape, factor, 0, middle)
    if fast:
        near, far = applied[:NEAR], applied[NEAR:]
        across = [to_y(part) for _, part in zip(far[::2], far[1::2])]
        joined = [join(part, back) for part, back in zip(far[::2], across)]
        joined[0], near[2] = lax.optimization_barrier((joined[0], near[2]))
        rows_kt, joined[1], near[1], near[3] = lax.optimization_barrier((rows_kt, joined[1], near[1], near[3]))
        got = [near[0]]
        for d in (2, 3, 1):
            got.append(over("hid", hid_count, lambda i, d=d: i ^ d)(near[d]))
        total = summed(got)
        halves = []
        at = 0
        for parts in joined:
            wide = parts[0].shape[1]
            arrived = [
                lax.ppermute(part, "hid", [(p, p ^ (NEAR + 2 * i)) for p in range(hid_count)])
                for i, part in enumerate(parts)
            ]
            halves.append(total[:, at : at + wide] + summed(arrived))
            at += wide
        total = jnp.concatenate(halves, axis=1)
    else:
        got = lax.all_to_all(applied[0], "hid", 0, 0)
        total = summed([got[d] for d in range(hid_count)])
    curvature_new = update(
        rows_kt, rows_n, held, curvature.shape, factor, middle, held.shape[0], curvature_new
    )
    return total[:each], curvature_new


def solution(mesh):
    in_specs = (P("col", "hid"), P("col", "hid"), P(None, "hid"), P(None, "hid"), P("hid", "col"))
    out_specs = (P("hid", "col"), P("hid", "col"))
    return jax.shard_map(
        per_device, mesh=mesh, in_specs=in_specs, out_specs=out_specs, check_vma=False
    )
```
